32 devices in a mesh: head: 4 (over x, core), ctx: 8 (over z, y).
Axes of the slice: x: 2, y: 2, z: 4, core: 2. Of those that a mesh axis runs over, the one named last changes fastest.
Arguments:
- query: bfloat16 [2048, 16384], P(('head', 'ctx')), may hold values from -5 to 5
- key: bfloat16 [2048, 1024], P(('head', 'ctx')), may hold values from -5 to 5
- value: bfloat16 [2048, 1024], P(('head', 'ctx')), may hold values from -6 to 6
- block_order: int32 [32], replicated, may hold values from 0 to 31, each once
Outputs:
- attended: bfloat16 [2048, 16384], P(('head', 'ctx'))
- log_norm_rows: float32 [2048, 128], P(('head', 'ctx'))
The draws below stay inside these ranges and needn't reach their ends.
All inputs are finite; a program needn't handle non-finite values.
Results may differ from the reference program's by a relative error of at most 0.0036.
Values may be sent and summed in bfloat16 or wider, within the bound.
A program may use at most 64 MiB of HBM per device.

```python
import math
import jax
import jax.numpy as jnp
from jax import lax

HQ = 128
KEY_VALUE_HEADS = 8
HEAD_DIMENSION = 128
BLOCK_ROWS = 64
SEQUENCE_TOKENS = 2048
N_HEAD = 4
N_CTX = 8


def draw_common(key, salt, width):
    fresh = jax.random.fold_in(key, salt)
    base = jnp.clip(jax.random.normal(fresh, (SEQUENCE_TOKENS, width), jnp.float32), -4.5, 4.5)
    return base


def draw_query(key, part):
    return draw_common(key, 3, HQ * HEAD_DIMENSION).astype(jnp.bfloat16)


def draw_key(key, part):
    return draw_common(key, 5, KEY_VALUE_HEADS * HEAD_DIMENSION).astype(jnp.bfloat16)


def shard_levels(own_key, dims, pieces, low, top_value):
    factor_of, own = 1.0, jax.random.fold_in(own_key, 6)
    for position, blocks in pieces:
        heights = jnp.exp(jax.random.uniform(jax.random.fold_in(own, position), (blocks,), jnp.float32, low / len(pieces), top_value / len(pieces)))
        factor_of = factor_of * jnp.repeat(heights, dims[position] // blocks).reshape([-1 if axis == position else 1 for axis in range(len(dims))])
    return factor_of


def noise(key, dims, scale, limit, shards=(), kind=jnp.bfloat16):
    values = jax.random.normal(key, dims, jnp.float32) * scale
    if len(shards) > 0:
        values = shard_levels(key, dims, shards, -0.22, 0.18) * values
    return jnp.clip(values, min=-limit, max=limit).astype(kind)


def setup_inputs(seed: int = 0) -> dict:
    key_list = jax.random.split(jax.random.key(seed), 5)
    return {
        "query": draw_query(jax.random.fold_in(key_list[4], 71), 0),
        "key": draw_key(jax.random.fold_in(key_list[4], 71), 0),
        "value": noise(key_list[2], (SEQUENCE_TOKENS, KEY_VALUE_HEADS * HEAD_DIMENSION), 1.0, 6.0, ((0, 32),)),
        "block_order": jax.random.permutation(key_list[3], SEQUENCE_TOKENS // BLOCK_ROWS).astype(jnp.int32),
    }


def shard_rows(array, shard):
    blocks = array.reshape(N_HEAD, N_CTX, BLOCK_ROWS, array.shape[-1])
    picked = lax.dynamic_index_in_dim(blocks, shard, 1, keepdims=False)
    return picked.reshape(N_HEAD * BLOCK_ROWS, array.shape[-1])

def partial_terms(queries, keys, values, query_positions, key_pos):
    rows = queries.shape[0]
    kv_heads = keys.shape[1] // HEAD_DIMENSION
    group = queries.shape[1] // HEAD_DIMENSION // kv_heads
    scale = 1.0 / math.sqrt(HEAD_DIMENSION)
    qf = queries.astype(jnp.float32).reshape(rows, kv_heads, group, HEAD_DIMENSION)
    kf = keys.astype(jnp.float32).reshape(-1, kv_heads, HEAD_DIMENSION)
    vf = values.astype(jnp.float32).reshape(-1, kv_heads, HEAD_DIMENSION)
    score_matrix = jnp.einsum('rhgd,khd->hgrk', qf, kf, precision=lax.Precision.HIGHEST) * scale
    visible = key_pos[None, :] <= query_positions[:, None]
    shifted = jnp.where(visible, score_matrix, -1e+30)
    peak = jnp.maximum(lax.optimization_barrier(jnp.max(shifted, axis=-1)), -10000.0)
    weights = jnp.exp(shifted - peak[..., None])
    total = lax.optimization_barrier(jnp.sum(weights, axis=-1))
    probs = weights.astype(jnp.bfloat16).astype(jnp.float32)
    acc = jnp.einsum('hgrk,khd->rhgd', probs, vf, precision=lax.Precision.HIGHEST)
    acc = acc.reshape(rows, kv_heads * group * HEAD_DIMENSION)
    peak = peak.transpose(2, 0, 1).reshape(rows, kv_heads * group)
    total = total.transpose(2, 0, 1).reshape(rows, kv_heads * group)
    return (peak, total, acc)

def combine(first, second):
    peak_a, total_a, acc_a = first
    peak_b, total_b, acc_b = second
    peak = jnp.maximum(peak_a, peak_b)
    factor_a = jnp.exp(peak_a - peak)
    factor_b = jnp.exp(peak_b - peak)
    total = total_a * factor_a + total_b * factor_b
    rows, heads = peak.shape
    acc = acc_a.reshape(rows, heads, -1) * factor_a[..., None] + acc_b.reshape(rows, heads, -1) * factor_b[..., None]
    result = (acc / total[..., None]).reshape(rows, -1)
    return (result, peak + jnp.log(total))

def reference(query, key, value, block_order):
    rows = jnp.arange(SEQUENCE_TOKENS, dtype=jnp.int32)
    pos = block_order[rows // BLOCK_ROWS].astype(jnp.int32) * BLOCK_ROWS + rows % BLOCK_ROWS
    pos_col = pos[:, None]

    def one_shard(shard):
        before = (shard - 1) % N_CTX
        queries = shard_rows(query, shard)
        local_positions = shard_rows(pos_col, shard)[:, 0]
        prev_pos = shard_rows(pos_col, before)[:, 0]
        own = partial_terms(queries, shard_rows(key, shard), shard_rows(value, shard), local_positions, local_positions)
        far = partial_terms(queries, shard_rows(key, before), shard_rows(value, before), local_positions, prev_pos)
        result, lse = combine(own, far)
        return (result.astype(jnp.bfloat16), lse)
    results, lses = lax.map(one_shard, jnp.arange(N_CTX, dtype=jnp.int32))
    attended = results.reshape(N_CTX, N_HEAD, BLOCK_ROWS, HQ * HEAD_DIMENSION).transpose(1, 0, 2, 3).reshape(SEQUENCE_TOKENS, HQ * HEAD_DIMENSION)
    log_norm_rows = lses.reshape(N_CTX, N_HEAD, BLOCK_ROWS, HQ).transpose(1, 0, 2, 3).reshape(SEQUENCE_TOKENS, HQ)
    return (attended, log_norm_rows)
```

```python
import functools
import math

import jax
import jax.numpy as jnp
from jax import lax
from jax.experimental import pallas as pl
from jax.experimental.pallas import tpu as pltpu
from jax.sharding import PartitionSpec as P

HEAD_DIMENSION = 128
MASKED = -1e30
FLOOR = -10000.0
GROUPS_PER_DOT = 4
MESH = pl.DeviceIdType.MESH


def kernel(
    n_head,
    n_ctx,
    order_ref,
    q_hbm,
    k_hbm,
    v_hbm,
    out_ref,
    lse_ref,
    qbuf,
    kbuf,
    vbuf,
    bias_ref,
    m_ref,
    l_ref,
    q_sem,
    own_sem,
    send_sem,
    recv_sem,
):
    d = HEAD_DIMENSION
    block = k_hbm.shape[0]
    kv_heads = k_hbm.shape[1] // d
    width = q_hbm.shape[1] // kv_heads
    group = width // d
    chips = n_head // 2
    slots = 2 * n_head
    n_keys = slots * block
    head = lax.axis_index("head")
    ctx = lax.axis_index("ctx")
    chip, core = lax.div(head, 2), lax.rem(head, 2)
    sibling_head = chip * 2 + (1 - core)
    next_ctx = lax.rem(ctx + 1, n_ctx)
    prev_ctx = lax.rem(ctx + n_ctx - 1, n_ctx)

    def chip_head(j):
        return lax.rem(chip + j, chips) * 2 + core

    def slot_of(p, j, s):
        return (p * chips + j) * 2 + s

    bufs = (kbuf, vbuf)

    def local_q(h):
        cols = pl.ds(pl.multiple_of(h * width, width), width)
        return pltpu.make_async_copy(q_hbm.at[:, cols], qbuf.at[h], q_sem.at[h])

    def local_kv(h, kv):
        cols = pl.ds(pl.multiple_of(h * d, d), d)
        src = (k_hbm, v_hbm)[kv]
        return pltpu.make_async_copy(src.at[:, cols], bufs[kv].at[h, 0], own_sem.at[h, kv])

    def remote(h, kv, src_slot, dst_slot, to_head, to_ctx):
        return pltpu.make_async_remote_copy(
            src_ref=bufs[kv].at[h, src_slot],
            dst_ref=bufs[kv].at[h, dst_slot],
            send_sem=send_sem.at[dst_slot, h, kv],
            recv_sem=recv_sem.at[dst_slot, h, kv],
            device_id=(to_head, to_ctx),
            device_id_type=MESH,
        )

    def to_sibling(h, kv, slot):
        return remote(h, kv, slot, slot + 1, sibling_head, ctx)

    def own_across(h, kv, j):
        return remote(h, kv, 0, slot_of(0, j, 0), chip_head(j), ctx)

    def own_onward(h, kv):
        return remote(h, kv, 0, slot_of(1, 0, 0), head, next_ctx)

    def relayed(h, kv, j):
        if kv == 0:
            return remote(h, 0, slot_of(1, 0, 0), slot_of(1, j, 0), chip_head(j), ctx)
        return remote(h, 1, slot_of(0, j, 0), slot_of(1, j, 0), head, next_ctx)

    def all_copies(h, kv):
        made = [own_onward(h, kv), to_sibling(h, kv, 0)]
        made += [own_across(h, kv, j) for j in range(1, chips)]
        made += [to_sibling(h, kv, slot_of(1, 0, 0))]
        for j in range(1, chips):
            made += [relayed(h, kv, j), to_sibling(h, kv, slot_of(0, j, 0)), to_sibling(h, kv, slot_of(1, j, 0))]
        return made

    for h in range(kv_heads):
        for kv in range(2):
            local_kv(h, kv).start()
    for h in range(kv_heads):
        local_q(h).start()

    barrier = pltpu.get_barrier_semaphore()
    pl.semaphore_signal(barrier, inc=1, device_id=(sibling_head, ctx), device_id_type=MESH)
    for j in range(1, chips):
        pl.semaphore_signal(barrier, inc=1, device_id=(chip_head(j), ctx), device_id_type=MESH)
    pl.semaphore_signal(barrier, inc=1, device_id=(head, next_ctx), device_id_type=MESH)
    pl.semaphore_signal(barrier, inc=1, device_id=(head, prev_ctx), device_id_type=MESH)

    rows = lax.broadcasted_iota(jnp.int32, (block, n_keys), 0)
    cols = lax.broadcasted_iota(jnp.int32, (block, n_keys), 1)
    key_slot, key_row = cols // block, cols % block
    key_block = jnp.zeros((block, n_keys), jnp.int32)
    for p in range(2):
        from_ctx = ctx if p == 0 else prev_ctx
        for j in range(chips):
            from_chip = lax.rem(chip + chips - j, chips)
            for s in range(2):
                from_head = from_chip * 2 + (core if s == 0 else 1 - core)
                stored = order_ref[from_head * n_ctx + from_ctx]
                key_block = jnp.where(key_slot == slot_of(p, j, s), stored, key_block)
    my_block = order_ref[head * n_ctx + ctx]
    visible = key_block * block + key_row <= my_block * block + rows
    bias_ref[...] = jnp.where(visible, 0.0, MASKED).astype(jnp.float32)
    m_ref[...] = jnp.zeros_like(m_ref)
    l_ref[...] = jnp.ones_like(l_ref)

    pl.semaphore_wait(barrier, chips + 2)

    def send_own(h):
        for kv in range(2):
            local_kv(h, kv).wait()
        for kv in range(2):
            for j in range(1, chips):
                own_across(h, kv, j).start()
            own_onward(h, kv).start()
            to_sibling(h, kv, 0).start()

    def first_hop(h):
        for kv in range(2):
            own_onward(h, kv).wait_recv()
            for j in range(1, chips):
                own_across(h, kv, j).wait_recv()
            for j in range(1, chips):
                relayed(h, kv, j).start()
            to_sibling(h, kv, slot_of(1, 0, 0)).start()
            for j in range(1, chips):
                to_sibling(h, kv, slot_of(0, j, 0)).start()

    def second_hop(h):
        for kv in range(2):
            for j in range(1, chips):
                relayed(h, kv, j).wait_recv()
                to_sibling(h, kv, slot_of(1, j, 0)).start()

    def last_hop(h):
        for kv in range(2):
            for p in range(2):
                for j in range(chips):
                    to_sibling(h, kv, slot_of(p, j, 0)).wait_recv()

    scale = 1.0 / math.sqrt(d)
    exp_scale = scale * math.log2(math.e)
    lane = lax.broadcasted_iota(jnp.int32, (block, lse_ref.shape[1]), 1)

    def attend(h):
        local_q(h).wait()
        k_h = kbuf[h].reshape(n_keys, d)
        v_h = vbuf[h].reshape(n_keys, d)
        v_ones = jnp.concatenate([v_h, jnp.ones_like(v_h)], axis=1)
        bias = bias_ref[...]
        m_all, l_all = m_ref[...], l_ref[...]
        for first in range(0, group, GROUPS_PER_DOT):
            members = range(first, min(first + GROUPS_PER_DOT, group))
            q = jnp.concatenate([qbuf[h, :, g * d : (g + 1) * d] for g in members], axis=0)
            s = lax.dot_general(q, k_h, (((1,), (1,)), ((), ())), preferred_element_type=jnp.float32)
            s = s.reshape(len(members), block, n_keys) + bias[None]
            m = jnp.maximum(jnp.max(s, axis=-1, keepdims=True), FLOOR / scale)
            probs = jnp.exp2((s - m) * exp_scale).astype(jnp.bfloat16)
            o = jnp.dot(
                probs.reshape(len(members) * block, n_keys), v_ones, preferred_element_type=jnp.float32
            )
            for i, g in enumerate(members):
                acc = o[i * block : (i + 1) * block, :d]
                total = o[i * block : (i + 1) * block, d:]
                start = pl.multiple_of(h * width + g * d, d)
                out_ref[:, pl.ds(start, d)] = (acc / total).astype(out_ref.dtype)
                here = lane == h * group + g
                m_all = jnp.where(here, m[i], m_all)
                l_all = jnp.where(here, total[:, :1], l_all)
        m_ref[...] = m_all
        l_ref[...] = l_all

    ahead = 3
    for h in range(min(ahead, kv_heads)):
        send_own(h)

    def stage(i, carry):
        t = i - 2

        @pl.when(t + 2 < kv_heads)
        def _():
            first_hop(t + 2)

        @pl.when(t + 2 + 1 < kv_heads)
        def _():
            @pl.when(t + 2 + 1 >= ahead)
            def _():
                send_own(t + 2 + 1)

        @pl.when(jnp.logical_and(t + 1 >= 0, t + 1 < kv_heads))
        def _():
            second_hop(t + 1)

        @pl.when(t >= 0)
        def _():
            last_hop(t)
            attend(t)

        return carry

    lax.fori_loop(0, kv_heads + 2, stage, 0)
    lse_ref[...] = m_ref[...] * scale + jnp.log(l_ref[...])

    def drain(h, carry):
        for kv in range(2):
            for copy in all_copies(h, kv):
                copy.wait_send()
        return carry

    lax.fori_loop(0, kv_heads, drain, 0)


def body(query, key, value, block_order):
    n_head = lax.axis_size("head")
    n_ctx = lax.axis_size("ctx")
    block, q_width = query.shape
    d = HEAD_DIMENSION
    kv_heads = key.shape[1] // d
    q_heads = q_width // d
    slots = 2 * n_head
    anywhere = pl.BlockSpec(memory_space=pl.ANY)
    vmem = pl.BlockSpec(memory_space=pltpu.VMEM)
    return pl.pallas_call(
        functools.partial(kernel, n_head, n_ctx),
        out_shape=(
            jax.ShapeDtypeStruct((block, q_width), jnp.bfloat16),
            jax.ShapeDtypeStruct((block, q_heads), jnp.float32),
        ),
        in_specs=[pl.BlockSpec(memory_space=pltpu.SMEM), anywhere, anywhere, anywhere],
        out_specs=(vmem, vmem),
        scratch_shapes=[
            pltpu.VMEM((kv_heads, block, q_width // kv_heads), jnp.bfloat16),
            pltpu.VMEM((kv_heads, slots, block, d), jnp.bfloat16),
            pltpu.VMEM((kv_heads, slots, block, d), jnp.bfloat16),
            pltpu.VMEM((block, slots * block), jnp.float32),
            pltpu.VMEM((block, q_heads), jnp.float32),
            pltpu.VMEM((block, q_heads), jnp.float32),
            pltpu.SemaphoreType.DMA((kv_heads,)),
            pltpu.SemaphoreType.DMA((kv_heads, 2)),
            pltpu.SemaphoreType.DMA((slots, kv_heads, 2)),
            pltpu.SemaphoreType.DMA((slots, kv_heads, 2)),
        ],
        compiler_params=pltpu.CompilerParams(collective_id=0, has_side_effects=True),
    )(block_order, query, key, value)


def solution(mesh):
    placed = (P(("head", "ctx"), None), P(("head", "ctx"), None), P(("head", "ctx"), None), P())
    return jax.shard_map(
        body,
        mesh=mesh,
        in_specs=placed,
        out_specs=(P(("head", "ctx"), None), P(("head", "ctx"), None)),
        check_vma=False,
    )
```

```python
import functools
import math

import jax
import jax.numpy as jnp
from jax import lax
from jax.experimental import pallas as pl
from jax.experimental.pallas import tpu as pltpu
from jax.sharding import PartitionSpec as P

HEAD_DIMENSION = 128
MASKED = -1e30
FLOOR = -10000.0
GROUPS_PER_DOT = 4
HEADS_PER_PIECE = 4
AHEAD = 2
VMEM_LIMIT = 24 * 1024 * 1024
MESH = pl.DeviceIdType.MESH


def key_bias(order_ref, block, n_head, n_ctx):
    head = lax.axis_index("head")
    ctx = lax.axis_index("ctx")
    chips = n_head // 2
    chip, core = lax.div(head, 2), lax.rem(head, 2)
    prev_ctx = lax.rem(ctx + n_ctx - 1, n_ctx)
    n_keys = 2 * n_head * block
    rows = lax.broadcasted_iota(jnp.int32, (block, n_keys), 0)
    cols = lax.broadcasted_iota(jnp.int32, (block, n_keys), 1)
    key_slot, key_row = cols // block, cols % block
    key_block = jnp.zeros((block, n_keys), jnp.int32)
    for p in range(2):
        from_ctx = ctx if p == 0 else prev_ctx
        for j in range(chips):
            from_chip = lax.rem(chip + chips - j, chips)
            for s in range(2):
                from_head = from_chip * 2 + (core if s == 0 else 1 - core)
                stored = order_ref[from_head * n_ctx + from_ctx]
                key_block = jnp.where(key_slot == (p * chips + j) * 2 + s, stored, key_block)
    my_block = order_ref[head * n_ctx + ctx]
    visible = key_block * block + key_row <= my_block * block + rows
    return jnp.where(visible, 0.0, MASKED).astype(jnp.float32)


def attend_head(h, group, q_ref, k_h, v_h, bias_ref, m_ref, l_ref, lane, put):
    d = HEAD_DIMENSION
    scale = 1.0 / math.sqrt(d)
    exp_scale = scale * math.log2(math.e)
    block, n_keys = bias_ref.shape
    v_ones = jnp.concatenate([v_h, jnp.ones_like(v_h)], axis=1)
    bias = bias_ref[...]
    m_all, l_all = m_ref[...], l_ref[...]
    for first in range(0, group, GROUPS_PER_DOT):
        members = range(first, min(first + GROUPS_PER_DOT, group))
        q = jnp.concatenate([q_ref[:, g * d : (g + 1) * d] for g in members], axis=0)
        s = lax.dot_general(q, k_h, (((1,), (1,)), ((), ())), preferred_element_type=jnp.float32)
        s = s.reshape(len(members), block, n_keys) + bias[None]
        m = jnp.maximum(jnp.max(s, axis=-1, keepdims=True), FLOOR / scale)
        probs = jnp.exp2((s - m) * exp_scale).astype(jnp.bfloat16)
        o = jnp.dot(
            probs.reshape(len(members) * block, n_keys), v_ones, preferred_element_type=jnp.float32
        )
        for i, g in enumerate(members):
            acc = o[i * block : (i + 1) * block, :d]
            total = o[i * block : (i + 1) * block, d:]
            put(g, (acc / total).astype(jnp.bfloat16))
            here = lane == h * group + g
            m_all = jnp.where(here, m[i], m_all)
            l_all = jnp.where(here, total[:, :1], l_all)
    m_ref[...] = m_all
    l_ref[...] = l_all


def finish_kernel(
    early,
    bias_ref,
    q_hbm,
    kv_ref,
    early_ref,
    stats_ref,
    out_hbm,
    lse_ref,
    qbuf,
    obuf,
    m_ref,
    l_ref,
    q_sem,
    out_sem,
):
    d = HEAD_DIMENSION
    late, _, _, block, piece = kv_ref.shape
    per_piece = piece // d
    n_late = late * per_piece
    n_early = early * per_piece
    width = q_hbm.shape[1] // (n_late + n_early)
    group = width // d
    n_keys = bias_ref.shape[1]

    def fetch(h):
        return pltpu.make_async_copy(
            q_hbm.at[:, pl.ds((n_early + h) * width, width)], qbuf.at[h], q_sem.at[h]
        )

    def store(h):
        return pltpu.make_async_copy(
            obuf.at[h], out_hbm.at[:, pl.ds((n_early + h) * width, width)], out_sem.at[h]
        )

    for h in range(n_late):
        fetch(h).start()
    ready = pltpu.make_async_copy(early_ref, out_hbm.at[:, pl.ds(0, n_early * width)], out_sem.at[n_late])
    ready.start()
    m_ref[...] = stats_ref[0]
    l_ref[...] = stats_ref[1]
    lane = lax.broadcasted_iota(jnp.int32, m_ref.shape, 1)
    for h in range(n_late):
        c, sub = h // per_piece, h % per_piece
        fetch(h).wait()
        k_h = kv_ref[c, :, 0, :, sub * d : (sub + 1) * d].reshape(n_keys, d)
        v_h = kv_ref[c, :, 1, :, sub * d : (sub + 1) * d].reshape(n_keys, d)

        def put(g, tile, h=h):
            obuf[h, :, g * d : (g + 1) * d] = tile

        attend_head(n_early + h, group, qbuf.at[h], k_h, v_h, bias_ref, m_ref, l_ref, lane, put)
        store(h).start()
    lse_ref[...] = m_ref[...] * (1.0 / math.sqrt(d)) + jnp.log(l_ref[...])
    for h in range(n_late):
        store(h).wait()
    ready.wait()


def kernel(
    n_head,
    n_ctx,
    order_ref,
    q_hbm,
    k_hbm,
    v_hbm,
    out_ref,
    late_ref,
    stats_ref,
    bias_ref,
    qbuf,
    kvearly,
    q_sem,
    own_sem,
    send_sem,
    recv_sem,
):
    d = HEAD_DIMENSION
    block = k_hbm.shape[0]
    early, piece = kvearly.shape[0], kvearly.shape[4]
    pieces = early + late_ref.shape[0]
    m_ref, l_ref = stats_ref.at[0], stats_ref.at[1]
    per_piece = piece // d
    kv_heads = pieces * per_piece
    width = q_hbm.shape[1] // kv_heads
    group = width // d
    chips = n_head // 2
    slots = 2 * n_head
    n_keys = slots * block
    head = lax.axis_index("head")
    ctx = lax.axis_index("ctx")
    chip, core = lax.div(head, 2), lax.rem(head, 2)
    sibling_head = chip * 2 + (1 - core)
    next_ctx = lax.rem(ctx + 1, n_ctx)
    prev_ctx = lax.rem(ctx + n_ctx - 1, n_ctx)

    def chip_head(j):
        return lax.rem(chip + j, chips) * 2 + core

    def slot_of(p, j, s):
        return (p * chips + j) * 2 + s

    def piece_of(c):
        return kvearly.at[c] if c < early else late_ref.at[c - early]

    def local_q(h):
        cols = pl.ds(pl.multiple_of(h * width, width), width)
        return pltpu.make_async_copy(q_hbm.at[:, cols], qbuf.at[h], q_sem.at[h])

    def local_kv(c, kv):
        cols = pl.ds(pl.multiple_of(c * piece, piece), piece)
        src = (k_hbm, v_hbm)[kv]
        return pltpu.make_async_copy(src.at[:, cols], piece_of(c).at[0, kv], own_sem.at[c, kv])

    def remote(c, src_slot, dst_slot, to_head, to_ctx):
        return pltpu.make_async_remote_copy(
            src_ref=piece_of(c).at[src_slot],
            dst_ref=piece_of(c).at[dst_slot],
            send_sem=send_sem.at[dst_slot, c, 0],
            recv_sem=recv_sem.at[dst_slot, c, 0],
            device_id=(to_head, to_ctx),
            device_id_type=MESH,
        )

    def to_sibling(c, slot):
        return remote(c, slot, slot + 1, sibling_head, ctx)

    def own_across(c, j):
        return remote(c, 0, slot_of(0, j, 0), chip_head(j), ctx)

    def own_onward(c):
        return remote(c, 0, slot_of(1, 0, 0), head, next_ctx)

    def relayed(c, kv, j):
        src_slot = (slot_of(1, 0, 0), slot_of(0, j, 0))[kv]
        dst_slot = slot_of(1, j, 0)
        return pltpu.make_async_remote_copy(
            src_ref=piece_of(c).at[src_slot, kv],
            dst_ref=piece_of(c).at[dst_slot, kv],
            send_sem=send_sem.at[dst_slot, c, kv],
            recv_sem=recv_sem.at[dst_slot, c, kv],
            device_id=((chip_head(j), ctx), (head, next_ctx))[kv],
            device_id_type=MESH,
        )

    def all_copies(c):
        made = [own_onward(c), to_sibling(c, 0)]
        made += [own_across(c, j) for j in range(1, chips)]
        made += [to_sibling(c, slot_of(1, 0, 0))]
        for j in range(1, chips):
            made += [relayed(c, 0, j), relayed(c, 1, j)]
            made += [to_sibling(c, slot_of(0, j, 0)), to_sibling(c, slot_of(1, j, 0))]
        return made

    for c in range(pieces):
        for kv in range(2):
            local_kv(c, kv).start()
    for h in range(early * per_piece):
        local_q(h).start()

    barrier = pltpu.get_barrier_semaphore()
    pl.semaphore_signal(barrier, inc=1, device_id=(sibling_head, ctx), device_id_type=MESH)
    for j in range(1, chips):
        pl.semaphore_signal(barrier, inc=1, device_id=(chip_head(j), ctx), device_id_type=MESH)
    pl.semaphore_signal(barrier, inc=1, device_id=(head, next_ctx), device_id_type=MESH)
    pl.semaphore_signal(barrier, inc=1, device_id=(head, prev_ctx), device_id_type=MESH)

    bias_ref[...] = key_bias(order_ref, block, n_head, n_ctx)
    m_ref[...] = jnp.zeros(m_ref.shape, jnp.float32)
    l_ref[...] = jnp.ones(l_ref.shape, jnp.float32)

    pl.semaphore_wait(barrier, chips + 2)

    def send_own(c):
        for kv in range(2):
            local_kv(c, kv).wait()
        for j in range(1, chips):
            own_across(c, j).start()
        own_onward(c).start()
        to_sibling(c, 0).start()

    def first_hop(c):
        own_onward(c).wait_recv()
        for j in range(1, chips):
            relayed(c, 0, j).start()
        for j in range(1, chips):
            own_across(c, j).wait_recv()
            relayed(c, 1, j).start()
        to_sibling(c, slot_of(1, 0, 0)).start()
        for j in range(1, chips):
            to_sibling(c, slot_of(0, j, 0)).start()

    def second_hop(c):
        for j in range(1, chips):
            for kv in range(2):
                relayed(c, kv, j).wait_recv()
            to_sibling(c, slot_of(1, j, 0)).start()

    def last_hop(c):
        for p in range(2):
            for j in range(chips):
                to_sibling(c, slot_of(p, j, 0)).wait_recv()

    stat_lane = lax.broadcasted_iota(jnp.int32, (block, m_ref.shape[1]), 1)

    def attend(c, sub):
        h = c * per_piece + sub
        local_q(h).wait()
        k_h = kvearly[c, :, 0, :, sub * d : (sub + 1) * d].reshape(n_keys, d)
        v_h = kvearly[c, :, 1, :, sub * d : (sub + 1) * d].reshape(n_keys, d)

        def put(g, tile):
            start = pl.multiple_of(h * width + g * d, d)
            out_ref[:, pl.ds(start, d)] = tile

        attend_head(h, group, qbuf.at[h], k_h, v_h, bias_ref, m_ref, l_ref, stat_lane, put)

    for c in range(min(AHEAD, pieces)):
        send_own(c)

    half = (per_piece + 1) // 2
    for i in range(pieces + 1):
        if i < pieces:
            first_hop(i)
        if i + AHEAD < pieces:
            send_own(i + AHEAD)
        if i == pieces:
            second_hop(i - 1)
        if 0 <= i - 2 < early:
            for sub in range(half, per_piece):
                attend(i - 2, sub)
        if 0 < i < pieces:
            second_hop(i - 1)
        if i > 0:
            last_hop(i - 1)
        if 0 <= i - 1 < early:
            for sub in range(half if i < pieces else per_piece):
                attend(i - 1, sub)
    for c in range(pieces):
        for copy in all_copies(c):
            copy.wait_send()


def body(query, key, value, block_order):
    n_head = lax.axis_size("head")
    n_ctx = lax.axis_size("ctx")
    block, q_width = query.shape
    d = HEAD_DIMENSION
    kv_heads = key.shape[1] // d
    q_heads = q_width // d
    slots = 2 * n_head
    per_piece = math.gcd(HEADS_PER_PIECE, kv_heads)
    pieces = kv_heads // per_piece
    per_piece = math.gcd(HEADS_PER_PIECE, kv_heads)
    pieces = kv_heads // per_piece
    late = 1
    early = pieces - late
    width = q_width // kv_heads
    piece_shape = (slots, 2, block, per_piece * d)
    anywhere = pl.BlockSpec(memory_space=pltpu.HBM)
    vmem = pl.BlockSpec(memory_space=pltpu.VMEM)
    smem = pl.BlockSpec(memory_space=pltpu.SMEM)
    query, key, value, block_order = (
        pltpu.with_memory_space_constraint(x, pltpu.HBM) for x in (query, key, value, block_order)
    )
    early_rows, late_kv, stats, bias = pl.pallas_call(
        functools.partial(kernel, n_head, n_ctx),
        out_shape=(
            jax.ShapeDtypeStruct((block, early * per_piece * width), jnp.bfloat16),
            jax.ShapeDtypeStruct((late, *piece_shape), jnp.bfloat16),
            jax.ShapeDtypeStruct((2, block, q_heads), jnp.float32),
            jax.ShapeDtypeStruct((block, slots * block), jnp.float32),
        ),
        in_specs=[smem, anywhere, anywhere, anywhere],
        out_specs=(vmem, vmem, vmem, vmem),
        scratch_shapes=[
            pltpu.VMEM((early * per_piece, block, width), jnp.bfloat16),
            pltpu.VMEM((early, *piece_shape), jnp.bfloat16),
            pltpu.SemaphoreType.DMA((early * per_piece,)),
            pltpu.SemaphoreType.DMA((pieces, 2)),
            pltpu.SemaphoreType.DMA((slots, pieces, 2)),
            pltpu.SemaphoreType.DMA((slots, pieces, 2)),
        ],
        compiler_params=pltpu.CompilerParams(
            collective_id=0, has_side_effects=True, vmem_limit_bytes=VMEM_LIMIT
        ),
    )(block_order, query, key, value)
    return pl.pallas_call(
        functools.partial(finish_kernel, early),
        out_shape=(
            jax.ShapeDtypeStruct((block, q_width), jnp.bfloat16),
            jax.ShapeDtypeStruct((block, q_heads), jnp.float32),
        ),
        in_specs=[vmem, anywhere, vmem, vmem, vmem],
        out_specs=(anywhere, vmem),
        scratch_shapes=[
            pltpu.VMEM((late * per_piece, block, width), jnp.bfloat16),
            pltpu.VMEM((late * per_piece, block, width), jnp.bfloat16),
            pltpu.VMEM((block, q_heads), jnp.float32),
            pltpu.VMEM((block, q_heads), jnp.float32),
            pltpu.SemaphoreType.DMA((late * per_piece,)),
            pltpu.SemaphoreType.DMA((late * per_piece + 1,)),
        ],
        compiler_params=pltpu.CompilerParams(vmem_limit_bytes=VMEM_LIMIT),
    )(bias, query, late_kv, early_rows, stats)


def solution(mesh):
    placed = (P(("head", "ctx"), None), P(("head", "ctx"), None), P(("head", "ctx"), None), P())
    return jax.shard_map(
        body,
        mesh=mesh,
        in_specs=placed,
        out_specs=(P(("head", "ctx"), None), P(("head", "ctx"), None)),
        check_vma=False,
    )
```

```python
import functools
import math

import jax
import jax.numpy as jnp
from jax import lax
from jax.experimental import pallas as pl
from jax.experimental.pallas import tpu as pltpu
from jax.sharding import PartitionSpec as P

HEAD_DIMENSION = 128
MASKED = -1e30
FLOOR = -10000.0
GROUPS_PER_DOT = 2
HEADS_PER_PIECE = 4
AHEAD = 2
VMEM_LIMIT = 24 * 1024 * 1024
MESH = pl.DeviceIdType.MESH


def key_bias(order_ref, block, n_head, n_ctx):
    head = lax.axis_index("head")
    ctx = lax.axis_index("ctx")
    chips = n_head // 2
    chip, core = lax.div(head, 2), lax.rem(head, 2)
    prev_ctx = lax.rem(ctx + n_ctx - 1, n_ctx)
    n_keys = 2 * n_head * block
    rows = lax.broadcasted_iota(jnp.int32, (block, n_keys), 0)
    cols = lax.broadcasted_iota(jnp.int32, (block, n_keys), 1)
    key_slot, key_row = cols // block, cols % block
    key_block = jnp.zeros((block, n_keys), jnp.int32)
    for p in range(2):
        from_ctx = ctx if p == 0 else prev_ctx
        for j in range(chips):
            from_chip = lax.rem(chip + chips - j, chips)
            for s in range(2):
                from_head = from_chip * 2 + (core if s == 0 else 1 - core)
                stored = order_ref[from_head * n_ctx + from_ctx]
                key_block = jnp.where(key_slot == (p * chips + j) * 2 + s, stored, key_block)
    my_block = order_ref[head * n_ctx + ctx]
    visible = key_block * block + key_row <= my_block * block + rows
    return jnp.where(visible, 0.0, MASKED).astype(jnp.float32)


def attend_head(h, group, q_ref, k_h, v_h, bias_ref, m_ref, l_ref, lane, put):
    d = HEAD_DIMENSION
    scale = 1.0 / math.sqrt(d)
    exp_scale = scale * math.log2(math.e)
    block, n_keys = bias_ref.shape
    v_ones = jnp.concatenate([v_h, jnp.ones_like(v_h)], axis=1)
    bias = bias_ref[...]
    m_all, l_all = m_ref[...], l_ref[...]
    for first in range(0, group, GROUPS_PER_DOT):
        members = range(first, min(first + GROUPS_PER_DOT, group))
        q = jnp.concatenate([q_ref[:, g * d : (g + 1) * d] for g in members], axis=0)
        s = lax.dot_general(q, k_h, (((1,), (1,)), ((), ())), preferred_element_type=jnp.float32)
        s = s.reshape(len(members), block, n_keys) + bias[None]
        m = jnp.maximum(jnp.max(s, axis=-1, keepdims=True), FLOOR / scale)
        probs = jnp.exp2((s - m) * exp_scale).astype(jnp.bfloat16)
        o = jnp.dot(
            probs.reshape(len(members) * block, n_keys), v_ones, preferred_element_type=jnp.float32
        )
        for i, g in enumerate(members):
            acc = o[i * block : (i + 1) * block, :d]
            total = o[i * block : (i + 1) * block, d:]
            put(g, (acc / total).astype(jnp.bfloat16))
            here = lane == h * group + g
            m_all = jnp.where(here, m[i], m_all)
            l_all = jnp.where(here, total[:, :1], l_all)
    m_ref[...] = m_all
    l_ref[...] = l_all


def finish_kernel(
    early,
    bias_ref,
    q_hbm,
    kv_ref,
    early_ref,
    stats_ref,
    out_hbm,
    lse_ref,
    qbuf,
    obuf,
    m_ref,
    l_ref,
    q_sem,
    out_sem,
):
    d = HEAD_DIMENSION
    late, _, _, block, piece = kv_ref.shape
    per_piece = piece // d
    n_late = late * per_piece
    n_early = early * per_piece
    width = q_hbm.shape[1] // (n_late + n_early)
    group = width // d
    n_keys = bias_ref.shape[1]

    def fetch(h):
        return pltpu.make_async_copy(
            q_hbm.at[:, pl.ds((n_early + h) * width, width)], qbuf.at[h], q_sem.at[h]
        )

    def store(h):
        return pltpu.make_async_copy(
            obuf.at[h], out_hbm.at[:, pl.ds((n_early + h) * width, width)], out_sem.at[h]
        )

    for h in range(n_late):
        fetch(h).start()
    ready = pltpu.make_async_copy(early_ref, out_hbm.at[:, pl.ds(0, n_early * width)], out_sem.at[n_late])
    ready.start()
    m_ref[...] = stats_ref[0]
    l_ref[...] = stats_ref[1]
    lane = lax.broadcasted_iota(jnp.int32, m_ref.shape, 1)
    for h in range(n_late):
        c, sub = h // per_piece, h % per_piece
        fetch(h).wait()
        k_h = kv_ref[c, :, 0, :, sub * d : (sub + 1) * d].reshape(n_keys, d)
        v_h = kv_ref[c, :, 1, :, sub * d : (sub + 1) * d].reshape(n_keys, d)

        def put(g, tile, h=h):
            obuf[h, :, g * d : (g + 1) * d] = tile

        attend_head(n_early + h, group, qbuf.at[h], k_h, v_h, bias_ref, m_ref, l_ref, lane, put)
        store(h).start()
    lse_ref[...] = m_ref[...] * (1.0 / math.sqrt(d)) + jnp.log(l_ref[...])
    for h in range(n_late):
        store(h).wait()
    ready.wait()


def kernel(
    n_head,
    n_ctx,
    order_ref,
    q_hbm,
    k_hbm,
    v_hbm,
    out_ref,
    late_ref,
    stats_ref,
    bias_ref,
    qbuf,
    kvearly,
    q_sem,
    own_sem,
    send_sem,
    recv_sem,
):
    d = HEAD_DIMENSION
    block = k_hbm.shape[0]
    early, piece = kvearly.shape[0], kvearly.shape[4]
    pieces = early + late_ref.shape[0]
    m_ref, l_ref = stats_ref.at[0], stats_ref.at[1]
    per_piece = piece // d
    kv_heads = pieces * per_piece
    width = q_hbm.shape[1] // kv_heads
    group = width // d
    chips = n_head // 2
    slots = 2 * n_head
    n_keys = slots * block
    head = lax.axis_index("head")
    ctx = lax.axis_index("ctx")
    chip, core = lax.div(head, 2), lax.rem(head, 2)
    sibling_head = chip * 2 + (1 - core)
    next_ctx = lax.rem(ctx + 1, n_ctx)
    prev_ctx = lax.rem(ctx + n_ctx - 1, n_ctx)

    def chip_head(j):
        return lax.rem(chip + j, chips) * 2 + core

    def slot_of(p, j, s):
        return (p * chips + j) * 2 + s

    def piece_of(c):
        return kvearly.at[c] if c < early else late_ref.at[c - early]

    def local_q(h):
        cols = pl.ds(pl.multiple_of(h * width, width), width)
        return pltpu.make_async_copy(q_hbm.at[:, cols], qbuf.at[h], q_sem.at[h])

    def local_kv(c, kv):
        cols = pl.ds(pl.multiple_of(c * piece, piece), piece)
        src = (k_hbm, v_hbm)[kv]
        return pltpu.make_async_copy(src.at[:, cols], piece_of(c).at[0, kv], own_sem.at[c, kv])

    def remote(c, src_slot, dst_slot, to_head, to_ctx):
        return pltpu.make_async_remote_copy(
            src_ref=piece_of(c).at[src_slot],
            dst_ref=piece_of(c).at[dst_slot],
            send_sem=send_sem.at[dst_slot, c, 0],
            recv_sem=recv_sem.at[dst_slot, c, 0],
            device_id=(to_head, to_ctx),
            device_id_type=MESH,
        )

    def to_sibling(c, slot):
        return remote(c, slot, slot + 1, sibling_head, ctx)

    def own_across(c, j):
        return remote(c, 0, slot_of(0, j, 0), chip_head(j), ctx)

    def own_onward(c):
        return remote(c, 0, slot_of(1, 0, 0), head, next_ctx)

    def relayed(c, kv, j):
        src_slot = (slot_of(1, 0, 0), slot_of(0, j, 0))[kv]
        dst_slot = slot_of(1, j, 0)
        return pltpu.make_async_remote_copy(
            src_ref=piece_of(c).at[src_slot, kv],
            dst_ref=piece_of(c).at[dst_slot, kv],
            send_sem=send_sem.at[dst_slot, c, kv],
            recv_sem=recv_sem.at[dst_slot, c, kv],
            device_id=((chip_head(j), ctx), (head, next_ctx))[kv],
            device_id_type=MESH,
        )

    def all_copies(c):
        made = [own_onward(c), to_sibling(c, 0)]
        made += [own_across(c, j) for j in range(1, chips)]
        made += [to_sibling(c, slot_of(1, 0, 0))]
        for j in range(1, chips):
            made += [relayed(c, 0, j), relayed(c, 1, j)]
            made += [to_sibling(c, slot_of(0, j, 0)), to_sibling(c, slot_of(1, j, 0))]
        return made

    for c in range(pieces):
        for kv in range(2):
            local_kv(c, kv).start()
    for h in range(early * per_piece):
        local_q(h).start()

    barrier = pltpu.get_barrier_semaphore()
    pl.semaphore_signal(barrier, inc=1, device_id=(sibling_head, ctx), device_id_type=MESH)
    for j in range(1, chips):
        pl.semaphore_signal(barrier, inc=1, device_id=(chip_head(j), ctx), device_id_type=MESH)
    pl.semaphore_signal(barrier, inc=1, device_id=(head, next_ctx), device_id_type=MESH)
    pl.semaphore_signal(barrier, inc=1, device_id=(head, prev_ctx), device_id_type=MESH)

    bias_ref[...] = key_bias(order_ref, block, n_head, n_ctx)
    m_ref[...] = jnp.zeros(m_ref.shape, jnp.float32)
    l_ref[...] = jnp.ones(l_ref.shape, jnp.float32)

    pl.semaphore_wait(barrier, chips + 2)

    def send_own(c):
        for kv in range(2):
            local_kv(c, kv).wait()
        for j in range(1, chips):
            own_across(c, j).start()
        own_onward(c).start()
        to_sibling(c, 0).start()

    def first_hop(c):
        own_onward(c).wait_recv()
        for j in range(1, chips):
            relayed(c, 0, j).start()
        for j in range(1, chips):
            own_across(c, j).wait_recv()
            relayed(c, 1, j).start()
        to_sibling(c, slot_of(1, 0, 0)).start()
        for j in range(1, chips):
            to_sibling(c, slot_of(0, j, 0)).start()

    def second_hop(c):
        for j in range(1, chips):
            for kv in range(2):
                relayed(c, kv, j).wait_recv()
            to_sibling(c, slot_of(1, j, 0)).start()

    def last_hop(c):
        for p in range(2):
            for j in range(chips):
                to_sibling(c, slot_of(p, j, 0)).wait_recv()

    stat_lane = lax.broadcasted_iota(jnp.int32, (block, m_ref.shape[1]), 1)

    def attend(c, sub):
        h = c * per_piece + sub
        local_q(h).wait()
        k_h = kvearly[c, :, 0, :, sub * d : (sub + 1) * d].reshape(n_keys, d)
        v_h = kvearly[c, :, 1, :, sub * d : (sub + 1) * d].reshape(n_keys, d)

        def put(g, tile):
            start = pl.multiple_of(h * width + g * d, d)
            out_ref[:, pl.ds(start, d)] = tile

        attend_head(h, group, qbuf.at[h], k_h, v_h, bias_ref, m_ref, l_ref, stat_lane, put)

    for c in range(min(AHEAD, pieces)):
        send_own(c)

    half = (per_piece + 1) // 2
    for i in range(pieces + 1):
        if i < pieces:
            first_hop(i)
        if i + AHEAD < pieces:
            send_own(i + AHEAD)
        if i == pieces:
            second_hop(i - 1)
        if 0 <= i - 2 < early:
            for sub in range(half, per_piece):
                attend(i - 2, sub)
        if 0 < i < pieces:
            second_hop(i - 1)
        if i > 0:
            last_hop(i - 1)
        if 0 <= i - 1 < early:
            for sub in range(half if i < pieces else per_piece):
                attend(i - 1, sub)
    for c in range(pieces):
        for copy in all_copies(c):
            copy.wait_send()


def body(query, key, value, block_order):
    n_head = lax.axis_size("head")
    n_ctx = lax.axis_size("ctx")
    block, q_width = query.shape
    d = HEAD_DIMENSION
    kv_heads = key.shape[1] // d
    q_heads = q_width // d
    slots = 2 * n_head
    per_piece = math.gcd(HEADS_PER_PIECE, kv_heads)
    pieces = kv_heads // per_piece
    per_piece = math.gcd(HEADS_PER_PIECE, kv_heads)
    pieces = kv_heads // per_piece
    late = 1
    early = pieces - late
    width = q_width // kv_heads
    piece_shape = (slots, 2, block, per_piece * d)
    anywhere = pl.BlockSpec(memory_space=pltpu.HBM)
    vmem = pl.BlockSpec(memory_space=pltpu.VMEM)
    smem = pl.BlockSpec(memory_space=pltpu.SMEM)
    query, key, value, block_order = (
        pltpu.with_memory_space_constraint(x, pltpu.HBM) for x in (query, key, value, block_order)
    )
    early_rows, late_kv, stats, bias = pl.pallas_call(
        functools.partial(kernel, n_head, n_ctx),
        out_shape=(
            jax.ShapeDtypeStruct((block, early * per_piece * width), jnp.bfloat16),
            jax.ShapeDtypeStruct((late, *piece_shape), jnp.bfloat16),
            jax.ShapeDtypeStruct((2, block, q_heads), jnp.float32),
            jax.ShapeDtypeStruct((block, slots * block), jnp.float32),
        ),
        in_specs=[smem, anywhere, anywhere, anywhere],
        out_specs=(vmem, vmem, vmem, vmem),
        scratch_shapes=[
            pltpu.VMEM((early * per_piece, block, width), jnp.bfloat16),
            pltpu.VMEM((early, *piece_shape), jnp.bfloat16),
            pltpu.SemaphoreType.DMA((early * per_piece,)),
            pltpu.SemaphoreType.DMA((pieces, 2)),
            pltpu.SemaphoreType.DMA((slots, pieces, 2)),
            pltpu.SemaphoreType.DMA((slots, pieces, 2)),
        ],
        compiler_params=pltpu.CompilerParams(
            collective_id=0, has_side_effects=True, vmem_limit_bytes=VMEM_LIMIT
        ),
    )(block_order, query, key, value)
    return pl.pallas_call(
        functools.partial(finish_kernel, early),
        out_shape=(
            jax.ShapeDtypeStruct((block, q_width), jnp.bfloat16),
            jax.ShapeDtypeStruct((block, q_heads), jnp.float32),
        ),
        in_specs=[vmem, anywhere, vmem, vmem, vmem],
        out_specs=(anywhere, vmem),
        scratch_shapes=[
            pltpu.VMEM((late * per_piece, block, width), jnp.bfloat16),
            pltpu.VMEM((late * per_piece, block, width), jnp.bfloat16),
            pltpu.VMEM((block, q_heads), jnp.float32),
            pltpu.VMEM((block, q_heads), jnp.float32),
            pltpu.SemaphoreType.DMA((late * per_piece,)),
            pltpu.SemaphoreType.DMA((late * per_piece + 1,)),
        ],
        compiler_params=pltpu.CompilerParams(vmem_limit_bytes=VMEM_LIMIT),
    )(bias, query, late_kv, early_rows, stats)


def solution(mesh):
    placed = (P(("head", "ctx"), None), P(("head", "ctx"), None), P(("head", "ctx"), None), P())
    return jax.shard_map(
        body,
        mesh=mesh,
        in_specs=placed,
        out_specs=(P(("head", "ctx"), None), P(("head", "ctx"), None)),
        check_vma=False,
    )
```
